32 devices in a mesh: clusters: 2 (over x), blk: 16 (over z, y, core).
Axes of the slice: x: 2, y: 2, z: 4, core: 2. Of those that a mesh axis runs over, the one named last changes fastest.
Arguments:
- positions: float32 [3, 65536], P(None, ('clusters', 'blk')), parts along dimension 1, may hold values from -6 to 6
- velocities: float32 [3, 65536], P(None, ('clusters', 'blk')), parts along dimension 1, may hold values from -6 to 6
- masses: float32 [65536], P(('clusters', 'blk')), parts along dimension 0, may hold values from 0.000390625 to 0.00390625
- active: int32 [8192], P(('clusters', 'blk')), parts along dimension 0, may hold values from 0 to 32767, as said below
Outputs:
- new_positions: float32 [3, 8192], P(None, ('clusters', 'blk')), parts along dimension 1
- new_velocities: float32 [3, 8192], P(None, ('clusters', 'blk')), parts along dimension 1
- accelerations: float32 [3, 8192], P(None, ('clusters', 'blk')), parts along dimension 1
- jerks: float32 [3, 8192], P(None, ('clusters', 'blk')), parts along dimension 1
The draws below stay inside these ranges and needn't reach their ends.
There are 2 independent parts, one for each index of `clusters`. The reference program is written for one: setup_inputs(seed, part) draws one part's arguments, and reference() takes and returns one part's arrays. A program takes and returns all parts, laid end to end along the dimension named above; each array names one. Nothing has to cross between parts.
Inputs may be any that keep to these rules, and one draw needn't show every extreme that they name: Entries b * 256 to (b + 1) * 256 - 1 of active name distinct stars among b * 2048 to (b + 1) * 2048 - 1, for every block b.
All inputs are finite; a program needn't handle non-finite values.
Results may differ from the reference program's by a relative error of at most 0.00023.
Values sent between devices are 32-bit elements; how exact they have to be, the bound alone decides.
A program may use at most 64 MiB of HBM per device.

```python
import math
import jax
import jax.numpy as jnp
from jax import lax

ACT_DEV = 256
STARS_DEV = 2048
ACTIVE = 4096
STARS = 32768
STEPS = 2


def draw_active(key, part):
    blocks = ACTIVE // ACT_DEV

    def one_block(index):
        block_key = jax.random.fold_in(key, index)
        inner = jax.random.permutation(block_key, STARS_DEV - 2)[:ACT_DEV - 2].astype(jnp.int32) + 1
        chosen = jnp.concatenate([inner, jnp.array([0, STARS_DEV - 1], jnp.int32)])
        order = jax.random.permutation(jax.random.fold_in(block_key, 7), ACT_DEV)
        return chosen[order] + index * STARS_DEV
    return jax.vmap(one_block)(jnp.arange(blocks, dtype=jnp.int32)).reshape(-1).astype(jnp.int32)


def levels(key, dims, shards, low, high):
    level = 1.0
    for position, shards_of in shards:
        draws = jax.random.uniform(jax.random.fold_in(jax.random.fold_in(key, 6), position), (shards_of,), jnp.float32, low / len(shards), high / len(shards))
        level = level * jnp.repeat(jnp.exp(draws), dims[position] // shards_of).reshape((-1,) + (1,) * (len(dims) - 1 - position))
    return level


def noise(rng, extent, scale, limit, split=(), kind=jnp.bfloat16):
    values = scale * jax.random.normal(rng, extent, jnp.float32)
    if split:
        values = values * levels(rng, extent, split, -0.22, 0.18)
    return jnp.clip(values, -limit, limit).astype(kind)


def setup_inputs(seed: int = 0, part: int = 0) -> dict:
    keys = jax.random.split(jax.random.key(seed), 5)
    part_splits = jax.random.split(jax.random.fold_in(keys[4], part), 5)
    positions = noise(part_splits[0], (3, STARS), 1.0, 6.0, ((1, 16),), jnp.float32)
    velocities = noise(part_splits[1], (3, STARS), 1.0, 6.0, ((1, 16),), jnp.float32)
    masses = jnp.clip(jnp.exp(math.log(0.00390625) - 2.3025851 * jax.random.uniform(part_splits[2], (STARS,), jnp.float32) ** levels(part_splits[2], (STARS,), ((0, 16),), -0.2, 0.2)), 0.000390625, 0.00390625)
    active = draw_active(jax.random.fold_in(jax.random.fold_in(keys[4], part), 71), part)
    return dict(positions=positions, velocities=velocities, masses=masses, active=active)


def pair_terms(target_pos, target_vel, source):
    separation = source[0:3, None, :] - target_pos[:, :, None]
    closing = source[3:6, None, :] - target_vel[:, :, None]
    squared = lax.optimization_barrier(jnp.sum(separation * separation, axis=0)) + 0.0025
    inverse = lax.rsqrt(squared)
    weight = source[6][None, :] * inverse * inverse * inverse
    radial = lax.optimization_barrier(jnp.sum(separation * closing, axis=0))
    accel = lax.optimization_barrier(jnp.sum(weight[None] * separation, axis=-1))
    jerk = lax.optimization_barrier(jnp.sum(weight[None] * (closing - 3.0 * (radial / squared)[None] * separation), axis=-1))
    return (accel, jerk)

def field(pos, vel, mass):
    source = jnp.concatenate([pos, vel, mass[None, :]], axis=0)
    blocks = ACTIVE // ACT_DEV
    stacked = jnp.concatenate([pos, vel], axis=0).reshape(6, blocks, ACT_DEV).transpose(1, 0, 2)

    def one_block(target):
        return pair_terms(target[0:3], target[3:6], source)
    accel, jerk = lax.map(one_block, stacked)
    accel = accel.transpose(1, 0, 2).reshape(3, ACTIVE)
    jerk = jerk.transpose(1, 0, 2).reshape(3, ACTIVE)
    return (accel, jerk)

def reference(positions, velocities, masses, active):
    time_step = 0.03125
    pos = jnp.take(positions, active, axis=1)
    vel = jnp.take(velocities, active, axis=1)
    mass = jnp.take(masses, active, axis=0)
    accel, jerk = field(pos, vel, mass)
    for section in range(STEPS):
        pred_pos = pos + time_step * vel + time_step ** 2 / 2.0 * accel + time_step ** 3 / 6.0 * jerk
        pred_vel = vel + time_step * accel + time_step ** 2 / 2.0 * jerk
        accel_new, jerk_new = field(pred_pos, pred_vel, mass)
        vel_new = vel + time_step / 2.0 * (accel + accel_new) + time_step ** 2 / 12.0 * (jerk - jerk_new)
        pos_new = pos + time_step / 2.0 * (vel + vel_new) + time_step ** 2 / 12.0 * (accel - accel_new)
        pos, vel, accel, jerk = (pos_new, vel_new, accel_new, jerk_new)
    return (pos, vel, accel, jerk)
```

```python
import functools

import jax
import jax.numpy as jnp
from jax import lax
from jax.experimental import pallas as pl
from jax.experimental.pallas import tpu as pltpu
from jax.sharding import PartitionSpec as P

STEPS = 2
TIME_STEP = 0.03125
ROWS = 32
SOFT = 0.0025
F32 = jnp.float32
BF16 = jnp.bfloat16


def split3(value):
    high = value.astype(BF16).astype(F32)
    rest = value - high
    middle = rest.astype(BF16).astype(F32)
    return high, middle, rest - middle


def kernel(
    n,
    pos_hbm,
    vel_hbm,
    mass_hbm,
    idx_hbm,
    out_ref,
    pos_ref,
    vel_ref,
    mass_ref,
    idx_ref,
    slots,
    target,
    feature,
    product,
    weights,
    right,
    total,
    in_sem,
    send_sem,
    recv_sem,
):
    me = lax.axis_index("blk")
    act = idx_ref.shape[1]
    stars = pos_ref.shape[1]

    half = n // 2
    chip = me // 2
    partner = me + 1 - 2 * lax.rem(me, 2)

    barrier = pltpu.get_barrier_semaphore()
    for k in range(1, n):
        pl.semaphore_signal(
            barrier,
            inc=1,
            device_id={"blk": lax.rem(me + k, n)},
            device_id_type=pl.DeviceIdType.MESH,
        )

    loads = [
        pltpu.make_async_copy(source, place, in_sem.at[k])
        for k, (source, place) in enumerate(
            [(idx_hbm, idx_ref), (pos_hbm, pos_ref), (vel_hbm, vel_ref), (mass_hbm, mass_ref)]
        )
    ]
    for load in loads:
        load.start()
    for load in loads:
        load.wait()

    row_id = lax.broadcasted_iota(jnp.int32, (8, act), 0)

    local_idx = idx_ref[...] - me * stars
    table = jnp.concatenate(
        [pos_ref[...], vel_ref[...], mass_ref[...], jnp.zeros((1, stars), F32)], axis=0
    )
    pieces = jnp.concatenate(split3(table), axis=0).astype(BF16)
    picked = (lax.broadcasted_iota(jnp.int32, (stars, act), 0) == local_idx).astype(F32).astype(BF16)
    found = jnp.dot(pieces, picked, preferred_element_type=F32)
    own = found[0:8] + found[8:16] + found[16:24]
    mass_rows = own[6:8]

    def chip_at(order):
        low = jnp.minimum(chip, half - 1 - chip)
        both = chip + ((order + 1) // 2) * (2 * lax.rem(order, 2) - 1)
        side = jnp.where(chip <= half - 1 - chip, order, half - 1 - order)
        return jnp.where(order <= 2 * low, both, side)

    def rows_at(step):
        return slice(0, 7 if step == 0 else 6)

    def send(step, peer):
        block = slots.at[step, me, rows_at(step)]
        return pltpu.make_async_remote_copy(
            src_ref=block,
            dst_ref=block,
            send_sem=send_sem.at[step],
            recv_sem=recv_sem.at[step, chip],
            device_id={"blk": peer},
            device_id_type=pl.DeviceIdType.MESH,
        )

    def arrival(step, first, count, source):
        blocks = slots.at[step, pl.ds(first, count), rows_at(step)]
        return pltpu.make_async_remote_copy(
            src_ref=blocks,
            dst_ref=blocks,
            send_sem=send_sem.at[step],
            recv_sem=recv_sem.at[step, source],
            device_id={"blk": partner},
            device_id_type=pl.DeviceIdType.MESH,
        )

    def dots(a, b):
        terms = a * b
        return terms[0:1] + terms[1:2] + terms[2:3]

    def stack(value, order, last):
        parts = split3(value)
        return jnp.concatenate([parts[k] for k in order] + [last, jnp.zeros_like(last)], axis=0)

    def prepare(step, source, centre, fine):
        for core in range(2):
            about = jnp.where(row_id < 6, slots[step, 2 * source + core] - centre, 0.0)
            factor = jnp.where(row_id == 6, 1.0, about)
            mass = slots[0, 2 * source + core, 6:7]
            right[core] = jnp.concatenate(split3(factor * mass), axis=0).astype(BF16)
            across = dots(about[0:3], about[3:6])
            square = dots(about[0:3], about[0:3])
            about = jnp.where(row_id == 6, across, jnp.where(row_id == 7, square, about))
            near = stack(about, (0, 0, 1, 1, 0, 2), jnp.ones_like(about)).astype(BF16)
            if fine:
                product[core, 0:act] = jnp.dot(
                    feature[act : 2 * act, :], near, preferred_element_type=F32
                )
            else:
                product[core] = jnp.dot(feature[...], near, preferred_element_type=F32)

    def weigh(step, source, fine):
        for core in range(2):
            for top in range(0, act, ROWS):
                rows = slice(top, top + ROWS)
                for side in range(0, act, 128):
                    lanes = slice(side, side + 128)
                    if fine:
                        d = [
                            slots[step, 2 * source + core, c : c + 1, lanes] - target[c, rows, :]
                            for c in range(3)
                        ]
                        squared = d[0] * d[0] + d[1] * d[1] + (d[2] * d[2] + SOFT)
                        radial = product[core, rows, lanes]
                    else:
                        squared = product[core, rows, lanes]
                        radial = product[core, act + top : act + top + ROWS, lanes]
                    inverse = lax.rsqrt(squared)
                    inverse2 = inverse * inverse
                    w = inverse2 * inverse
                    z = w * inverse2 * radial
                    for k, value in enumerate([w, z]):
                        high = value.astype(BF16)
                        weights[k, core, rows, lanes] = high
                        if fine:
                            low = (value - high.astype(F32)).astype(BF16)
                            weights[2 + k, core, rows, lanes] = low

    def reduce(fine):
        for core in range(2):
            for k in range(4 if fine else 2):
                total[k % 2] += lax.dot_general(
                    right[core],
                    weights[k, core],
                    (((1,), (1,)), ((), ())),
                    preferred_element_type=F32,
                )

    def field(step, own):
        fine = step == STEPS
        slots[step, me] = own
        if step == 0:
            pl.semaphore_wait(barrier, n - 1)
        send(step, partner).start()
        for order in range(1, half):
            there = 2 * chip_at(order)
            send(step, there).start()
            send(step, there + 1).start()

        centre = jnp.where(row_id[:, 0:1] < 6, jnp.mean(own, axis=1, keepdims=True), 0.0)
        about = own - centre
        none, one = jnp.zeros((1, act), F32), jnp.ones((1, act), F32)
        pad = jnp.zeros((5, act), F32)
        if fine:
            columns = own[0:8].T
            for c in range(3):
                target[c] = jnp.broadcast_to(columns[:, c : c + 1], (act, 128))
        else:
            square = dots(about[0:3], about[0:3]) + SOFT
            value = jnp.concatenate([-2.0 * about[0:3], none, none, none, none, one], axis=0)
            last = jnp.concatenate(list(split3(square)) + [pad], axis=0)
            feature[0:act, :] = stack(value, (0, 1, 0, 1, 2, 0), last).T.astype(BF16)
        across = dots(about[0:3], about[3:6])
        value = jnp.concatenate([-about[3:6], -about[0:3], one, none], axis=0)
        last = jnp.concatenate(list(split3(across)) + [pad], axis=0)
        feature[act : 2 * act, :] = stack(value, (0, 1, 0, 1, 2, 0), last).T.astype(BF16)
        total[...] = jnp.zeros_like(total)

        arrival(step, partner, 1, chip).wait_recv()
        prepare(step, chip, centre, fine)
        weigh(step, chip, fine)

        @pl.loop(1, half)
        def _(order):
            source = chip_at(order)
            arrival(step, 2 * source, 2, source).wait_recv()
            reduce(fine)
            prepare(step, source, centre, fine)
            weigh(step, source, fine)

        reduce(fine)
        plain, scaled = [total[k][0:8] + total[k][8:16] + total[k][16:24] for k in range(2)]
        accel = plain[0:3] - about[0:3] * plain[6:7]
        jerk = (
            plain[3:6]
            - about[3:6] * plain[6:7]
            - 3.0 * (scaled[0:3] - about[0:3] * scaled[6:7])
        )
        return accel, jerk

    pos, vel = own[0:3], own[3:6]
    accel, jerk = field(0, own)
    h = TIME_STEP
    for step in range(STEPS):
        pred_pos = pos + h * vel + h**2 / 2.0 * accel + h**3 / 6.0 * jerk
        pred_vel = vel + h * accel + h**2 / 2.0 * jerk
        accel_new, jerk_new = field(
            step + 1, jnp.concatenate([pred_pos, pred_vel, mass_rows], axis=0)
        )
        vel_new = vel + h / 2.0 * (accel + accel_new) + h**2 / 12.0 * (jerk - jerk_new)
        pos = pos + h / 2.0 * (vel + vel_new) + h**2 / 12.0 * (accel - accel_new)
        vel, accel, jerk = vel_new, accel_new, jerk_new
    out_ref[...] = jnp.concatenate([pos, vel, accel, jerk], axis=0)

    for step in range(STEPS + 1):
        arrival(step, 0, n - 1, 0).wait_send()


def solution(mesh):
    n = mesh.shape["blk"]

    def shards(positions, velocities, masses, active):
        act, stars = active.shape[0], masses.shape[0]
        hbm = pl.BlockSpec(memory_space=pltpu.HBM)
        packed = pl.pallas_call(
            functools.partial(kernel, n),
            out_shape=jax.ShapeDtypeStruct((12, act), F32),
            in_specs=[hbm] * 4,
            out_specs=pl.BlockSpec(memory_space=pltpu.VMEM),
            scratch_shapes=[
                pltpu.VMEM((3, stars), F32),
                pltpu.VMEM((3, stars), F32),
                pltpu.VMEM((1, stars), F32),
                pltpu.VMEM((1, act), jnp.int32),
                pltpu.VMEM((STEPS + 1, n, 8, act), F32),
                pltpu.VMEM((3, act, 128), F32),
                pltpu.VMEM((2 * act, 64), BF16),
                pltpu.VMEM((2, 2 * act, act), F32),
                pltpu.VMEM((4, 2, act, act), BF16),
                pltpu.VMEM((2, 24, act), BF16),
                pltpu.VMEM((2, 24, act), F32),
                pltpu.SemaphoreType.DMA((4,)),
                pltpu.SemaphoreType.DMA((STEPS + 1,)),
                pltpu.SemaphoreType.DMA((STEPS + 1, n // 2)),
            ],
            compiler_params=pltpu.CompilerParams(
                collective_id=0, has_side_effects=True, vmem_limit_bytes=24 * 1024 * 1024
            ),
        )(positions, velocities, masses.reshape(1, -1), active.reshape(1, -1))
        return packed[0:3], packed[3:6], packed[6:9], packed[9:12]

    spec = P(None, ("clusters", "blk"))
    flat = P(("clusters", "blk"))
    return jax.shard_map(
        shards,
        mesh=mesh,
        in_specs=(spec, spec, flat, flat),
        out_specs=(spec, spec, spec, spec),
        check_vma=False,
    )
```

```python
import functools

import jax
import jax.numpy as jnp
from jax import lax
from jax.experimental import pallas as pl
from jax.experimental.pallas import tpu as pltpu
from jax.sharding import PartitionSpec as P

STEPS = 2
TIME_STEP = 0.03125
ROWS = 32
SOFT = 0.0025
F32 = jnp.float32
BF16 = jnp.bfloat16


def split3(value):
    high = value.astype(BF16).astype(F32)
    rest = value - high
    middle = rest.astype(BF16).astype(F32)
    return high, middle, rest - middle


def kernel(
    n,
    pos_hbm,
    vel_hbm,
    mass_hbm,
    idx_hbm,
    out_ref,
    pos_ref,
    vel_ref,
    mass_ref,
    idx_ref,
    slots,
    target,
    across_rows,
    feature,
    product,
    weights,
    right,
    total,
    in_sem,
    send_sem,
    recv_sem,
):
    me = lax.axis_index("blk")
    act = idx_ref.shape[1]
    stars = pos_ref.shape[1]

    half = n // 2
    chip = me // 2
    partner = me + 1 - 2 * lax.rem(me, 2)

    barrier = pltpu.get_barrier_semaphore()
    for k in range(1, n):
        pl.semaphore_signal(
            barrier,
            inc=1,
            device_id={"blk": lax.rem(me + k, n)},
            device_id_type=pl.DeviceIdType.MESH,
        )

    loads = [
        pltpu.make_async_copy(source, place, in_sem.at[k])
        for k, (source, place) in enumerate(
            [(idx_hbm, idx_ref), (pos_hbm, pos_ref), (vel_hbm, vel_ref), (mass_hbm, mass_ref)]
        )
    ]
    for load in loads:
        load.start()
    for load in loads:
        load.wait()

    row_id = lax.broadcasted_iota(jnp.int32, (8, act), 0)

    local_idx = idx_ref[...] - me * stars
    table = jnp.concatenate(
        [pos_ref[...], vel_ref[...], mass_ref[...], jnp.zeros((1, stars), F32)], axis=0
    )
    pieces = jnp.concatenate(split3(table), axis=0).astype(BF16)
    picked = (lax.broadcasted_iota(jnp.int32, (stars, act), 0) == local_idx).astype(F32).astype(BF16)
    found = jnp.dot(pieces, picked, preferred_element_type=F32)
    own = found[0:8] + found[8:16] + found[16:24]
    mass_rows = own[6:8]

    def chip_at(order):
        low = jnp.minimum(chip, half - 1 - chip)
        both = chip + ((order + 1) // 2) * (2 * lax.rem(order, 2) - 1)
        side = jnp.where(chip <= half - 1 - chip, order, half - 1 - order)
        return jnp.where(order <= 2 * low, both, side)

    def rows_at(step):
        return slice(0, 7 if step == 0 else 6)

    def send(step, peer):
        block = slots.at[step, me, rows_at(step)]
        return pltpu.make_async_remote_copy(
            src_ref=block,
            dst_ref=block,
            send_sem=send_sem.at[step],
            recv_sem=recv_sem.at[step, chip],
            device_id={"blk": peer},
            device_id_type=pl.DeviceIdType.MESH,
        )

    def arrival(step, first, count, source):
        blocks = slots.at[step, pl.ds(first, count), rows_at(step)]
        return pltpu.make_async_remote_copy(
            src_ref=blocks,
            dst_ref=blocks,
            send_sem=send_sem.at[step],
            recv_sem=recv_sem.at[step, source],
            device_id={"blk": partner},
            device_id_type=pl.DeviceIdType.MESH,
        )

    def dots(a, b):
        terms = a * b
        return terms[0:1] + terms[1:2] + terms[2:3]

    def stack(value, order, last):
        parts = split3(value)
        return jnp.concatenate([parts[k] for k in order] + last, axis=0)

    def prepare(step, source, centre, fine):
        for side in range(2):
            about = jnp.where(row_id < 6, slots[step, 2 * source + side] - centre, 0.0)
            factor = jnp.where(row_id == 6, 1.0, about)
            mass = slots[0, 2 * source + side, 6:7]
            right[side] = jnp.concatenate(split3(factor * mass), axis=0).astype(BF16)
            across = dots(about[0:3], about[3:6])
            square = dots(about[0:3], about[0:3])
            about = jnp.where(row_id == 6, across, jnp.where(row_id == 7, square, about))
            near = stack(about, (0, 0, 1, 1, 0, 2), [jnp.ones_like(about), jnp.zeros_like(about)])
            if fine:
                product[side, :, 0:act] = jnp.dot(
                    across_rows[...], near.astype(BF16), preferred_element_type=F32
                )
            else:
                product[side] = jnp.dot(
                    near.T.astype(BF16), feature[...], preferred_element_type=F32
                )

    def weigh(step, source, fine):
        for side in range(2):
            for top in range(0, act, ROWS):
                rows = slice(top, top + ROWS)
                for left in range(0, act, 128):
                    lanes = slice(left, left + 128)
                    if fine:
                        d = [
                            slots[step, 2 * source + side, c : c + 1, lanes] - target[c, rows, :]
                            for c in range(3)
                        ]
                        squared = d[0] * d[0] + d[1] * d[1] + (d[2] * d[2] + SOFT)
                        radial = product[side, rows, lanes]
                    else:
                        squared = product[side, rows, lanes]
                        radial = product[side, rows, act + left : act + left + 128]
                    inverse = lax.rsqrt(squared)
                    inverse2 = inverse * inverse
                    w = inverse2 * inverse
                    z = w * inverse2 * radial
                    for k, value in enumerate([w, z]):
                        high = value.astype(BF16)
                        weights[k, side, rows, lanes] = high
                        if fine:
                            low = (value - high.astype(F32)).astype(BF16)
                            weights[2 + k, side, rows, lanes] = low

    def reduce(fine):
        for side in range(2):
            for k in range(4 if fine else 2):
                total[k % 2] += lax.dot_general(
                    right[side],
                    weights[k, side],
                    (((1,), (1 if fine else 0,)), ((), ())),
                    preferred_element_type=F32,
                )

    def field(step, own):
        fine = step == STEPS
        slots[step, me] = own
        if step == 0:
            pl.semaphore_wait(barrier, n - 1)
        send(step, partner).start()
        for order in range(1, half):
            there = 2 * chip_at(order)
            send(step, there).start()
            send(step, there + 1).start()

        centre = jnp.where(row_id[:, 0:1] < 6, jnp.mean(own, axis=1, keepdims=True), 0.0)
        about = own - centre
        none, one = jnp.zeros((1, act), F32), jnp.ones((1, act), F32)
        pad = jnp.zeros((13, act), F32)
        if not fine:
            square = dots(about[0:3], about[0:3]) + SOFT
            value = jnp.concatenate([-2.0 * about[0:3], none, none, none, none, one], axis=0)
            last = [*split3(square), pad]
            feature[:, 0:act] = stack(value, (0, 1, 0, 1, 2, 0), last).astype(BF16)
        across = dots(about[0:3], about[3:6])
        value = jnp.concatenate([-about[3:6], -about[0:3], one, none], axis=0)
        last = [*split3(across), pad]
        if fine:
            across_rows[...] = stack(value, (0, 1, 0, 1, 2, 0), last).T.astype(BF16)
            columns = own.T
            for c in range(3):
                target[c] = jnp.broadcast_to(columns[:, c : c + 1], (act, 128))
        else:
            feature[:, act : 2 * act] = stack(value, (0, 1, 0, 1, 2, 0), last).astype(BF16)
        total[...] = jnp.zeros_like(total)

        arrival(step, partner, 1, chip).wait_recv()
        prepare(step, chip, centre, fine)
        weigh(step, chip, fine)

        @pl.loop(1, half)
        def _(order):
            source = chip_at(order)
            arrival(step, 2 * source, 2, source).wait_recv()
            reduce(fine)
            prepare(step, source, centre, fine)
            weigh(step, source, fine)

        reduce(fine)
        plain, scaled = [total[k][0:8] + total[k][8:16] + total[k][16:24] for k in range(2)]
        accel = plain[0:3] - about[0:3] * plain[6:7]
        jerk = (
            plain[3:6]
            - about[3:6] * plain[6:7]
            - 3.0 * (scaled[0:3] - about[0:3] * scaled[6:7])
        )
        return accel, jerk

    pos, vel = own[0:3], own[3:6]
    accel, jerk = field(0, own)
    h = TIME_STEP
    for step in range(STEPS):
        pred_pos = pos + h * vel + h**2 / 2.0 * accel + h**3 / 6.0 * jerk
        pred_vel = vel + h * accel + h**2 / 2.0 * jerk
        accel_new, jerk_new = field(
            step + 1, jnp.concatenate([pred_pos, pred_vel, mass_rows], axis=0)
        )
        vel_new = vel + h / 2.0 * (accel + accel_new) + h**2 / 12.0 * (jerk - jerk_new)
        pos = pos + h / 2.0 * (vel + vel_new) + h**2 / 12.0 * (accel - accel_new)
        vel, accel, jerk = vel_new, accel_new, jerk_new
    out_ref[...] = jnp.concatenate([pos, vel, accel, jerk], axis=0)

    for step in range(STEPS + 1):
        arrival(step, 0, n - 1, 0).wait_send()


def solution(mesh):
    n = mesh.shape["blk"]

    def shards(positions, velocities, masses, active):
        act, stars = active.shape[0], masses.shape[0]
        hbm = pl.BlockSpec(memory_space=pltpu.HBM)
        positions, velocities, masses, active = [
            pltpu.with_memory_space_constraint(value, pltpu.HBM)
            for value in (positions, velocities, masses.reshape(1, -1), active.reshape(1, -1))
        ]
        packed = pl.pallas_call(
            functools.partial(kernel, n),
            out_shape=jax.ShapeDtypeStruct((12, act), F32),
            in_specs=[hbm] * 4,
            out_specs=pl.BlockSpec(memory_space=pltpu.VMEM),
            scratch_shapes=[
                pltpu.VMEM((3, stars), F32),
                pltpu.VMEM((3, stars), F32),
                pltpu.VMEM((1, stars), F32),
                pltpu.VMEM((1, act), jnp.int32),
                pltpu.VMEM((STEPS + 1, n, 8, act), F32),
                pltpu.VMEM((3, act, 128), F32),
                pltpu.VMEM((act, 64), BF16),
                pltpu.VMEM((64, 2 * act), BF16),
                pltpu.VMEM((2, act, 2 * act), F32),
                pltpu.VMEM((4, 2, act, act), BF16),
                pltpu.VMEM((2, 24, act), BF16),
                pltpu.VMEM((2, 24, act), F32),
                pltpu.SemaphoreType.DMA((4,)),
                pltpu.SemaphoreType.DMA((STEPS + 1,)),
                pltpu.SemaphoreType.DMA((STEPS + 1, n // 2)),
            ],
            compiler_params=pltpu.CompilerParams(
                collective_id=0, has_side_effects=True, vmem_limit_bytes=24 * 1024 * 1024
            ),
        )(positions, velocities, masses, active)
        return packed[0:3], packed[3:6], packed[6:9], packed[9:12]

    spec = P(None, ("clusters", "blk"))
    flat = P(("clusters", "blk"))
    return jax.shard_map(
        shards,
        mesh=mesh,
        in_specs=(spec, spec, flat, flat),
        out_specs=(spec, spec, spec, spec),
        check_vma=False,
    )
```

```python
import functools

import jax
import jax.numpy as jnp
from jax import lax
from jax.experimental import pallas as pl
from jax.experimental.pallas import tpu as pltpu
from jax.sharding import PartitionSpec as P

STEPS = 2
TIME_STEP = 0.03125
ROWS = 16
SOFT = 0.0025
F32 = jnp.float32
BF16 = jnp.bfloat16


def split3(value):
    high = value.astype(BF16).astype(F32)
    rest = value - high
    middle = rest.astype(BF16).astype(F32)
    return high, middle, rest - middle


def kernel(
    n,
    pos_hbm,
    vel_hbm,
    mass_hbm,
    idx_hbm,
    out_ref,
    pos_ref,
    vel_ref,
    mass_ref,
    idx_ref,
    slots,
    target,
    across_rows,
    feature,
    product,
    weights,
    right,
    total,
    in_sem,
    send_sem,
    recv_sem,
):
    me = lax.axis_index("blk")
    act = idx_ref.shape[1]
    stars = pos_ref.shape[1]

    half = n // 2
    chip = me // 2
    partner = me + 1 - 2 * lax.rem(me, 2)

    barrier = pltpu.get_barrier_semaphore()
    for k in range(1, n):
        pl.semaphore_signal(
            barrier,
            inc=1,
            device_id={"blk": lax.rem(me + k, n)},
            device_id_type=pl.DeviceIdType.MESH,
        )

    loads = [
        pltpu.make_async_copy(source, place, in_sem.at[k])
        for k, (source, place) in enumerate(
            [(idx_hbm, idx_ref), (pos_hbm, pos_ref), (vel_hbm, vel_ref), (mass_hbm, mass_ref)]
        )
    ]
    for load in loads:
        load.start()
    for load in loads:
        load.wait()

    row_id = lax.broadcasted_iota(jnp.int32, (8, act), 0)
    weights[...] = jnp.zeros_like(weights)

    local_idx = idx_ref[...] - me * stars
    table = jnp.concatenate(
        [pos_ref[...], vel_ref[...], mass_ref[...], jnp.zeros((1, stars), F32)], axis=0
    )
    pieces = jnp.concatenate(split3(table), axis=0).astype(BF16)
    picked = (lax.broadcasted_iota(jnp.int32, (stars, act), 0) == local_idx).astype(F32).astype(BF16)
    found = jnp.dot(pieces, picked, preferred_element_type=F32)
    own = found[0:8] + found[8:16] + found[16:24]
    mass_rows = own[6:8]

    def chip_at(order):
        low = jnp.minimum(chip, half - 1 - chip)
        both = chip + ((order + 1) // 2) * (2 * lax.rem(order, 2) - 1)
        side = jnp.where(chip <= half - 1 - chip, order, half - 1 - order)
        return jnp.where(order <= 2 * low, both, side)

    peers = [2 * chip_at(order) for order in range(1, half)]

    def rows_at(step):
        return slice(0, 7 if step == 0 else 6)

    def send(step, peer):
        block = slots.at[step, me, rows_at(step)]
        return pltpu.make_async_remote_copy(
            src_ref=block,
            dst_ref=block,
            send_sem=send_sem.at[step],
            recv_sem=recv_sem.at[step, chip],
            device_id={"blk": peer},
            device_id_type=pl.DeviceIdType.MESH,
        )

    def arrival(step, first, count, source):
        blocks = slots.at[step, pl.ds(first, count), rows_at(step)]
        return pltpu.make_async_remote_copy(
            src_ref=blocks,
            dst_ref=blocks,
            send_sem=send_sem.at[step],
            recv_sem=recv_sem.at[step, source],
            device_id={"blk": partner},
            device_id_type=pl.DeviceIdType.MESH,
        )

    def dots(a, b):
        terms = a * b
        return terms[0:1] + terms[1:2] + terms[2:3]

    def stack(value, order, last):
        parts = split3(value)
        return jnp.concatenate([parts[k] for k in order] + last, axis=0)

    def prepare(step, source, centre, fine):
        for side in range(2):
            about = jnp.where(row_id < 6, slots[step, 2 * source + side] - centre, 0.0)
            factor = jnp.where(row_id == 6, 1.0, about)
            mass = slots[0, 2 * source + side, 6:7]
            right[side] = jnp.concatenate(split3(factor * mass), axis=0).astype(BF16)
            across = dots(about[0:3], about[3:6])
            square = dots(about[0:3], about[0:3])
            about = jnp.where(row_id == 6, across, jnp.where(row_id == 7, square, about))
            near = stack(about, (0, 0, 1, 1, 0, 2), [jnp.ones_like(about), jnp.zeros_like(about)])
            if fine:
                product[side, :, 0:act] = jnp.dot(
                    across_rows[...], near.astype(BF16), preferred_element_type=F32
                )
            else:
                product[side] = jnp.dot(
                    near.T.astype(BF16), feature[...], preferred_element_type=F32
                )

    def weigh(step, source, fine):
        for side in range(2):
            for top in range(0, act, ROWS):
                rows = slice(top, top + ROWS)
                for left in range(0, act, 128):
                    lanes = slice(left, left + 128)
                    if fine:
                        d = [
                            slots[step, 2 * source + side, c : c + 1, lanes] - target[c, rows, :]
                            for c in range(3)
                        ]
                        squared = d[0] * d[0] + d[1] * d[1] + (d[2] * d[2] + SOFT)
                        radial = product[side, rows, lanes]
                    else:
                        squared = product[side, rows, lanes]
                        radial = product[side, rows, act + left : act + left + 128]
                    inverse = lax.rsqrt(squared)
                    inverse2 = inverse * inverse
                    w = inverse2 * inverse
                    z = w * inverse2 * radial
                    for k, value in enumerate([w, z]):
                        high = value.astype(BF16)
                        weights[k, side, rows, lanes] = high
                        if fine:
                            low = (value - high.astype(F32)).astype(BF16)
                            weights[2 + k, side, rows, lanes] = low

    def reduce(fine):
        for side in range(2):
            for k in range(4 if fine else 2):
                total[k % 2] += lax.dot_general(
                    right[side],
                    weights[k, side],
                    (((1,), (1 if fine else 0,)), ((), ())),
                    preferred_element_type=F32,
                )

    def field(step, own):
        fine = step == STEPS
        slots[step, me] = own
        if step == 0:
            pl.semaphore_wait(barrier, n - 1)
        send(step, partner).start()
        for there in peers:
            send(step, there).start()
            send(step, there + 1).start()

        centre = jnp.where(row_id[:, 0:1] < 6, jnp.mean(own, axis=1, keepdims=True), 0.0)
        about = own - centre
        none, one = jnp.zeros((1, act), F32), jnp.ones((1, act), F32)
        pad = jnp.zeros((13, act), F32)
        if not fine:
            square = dots(about[0:3], about[0:3]) + SOFT
            value = jnp.concatenate([-2.0 * about[0:3], none, none, none, none, one], axis=0)
            last = [*split3(square), pad]
            feature[:, 0:act] = stack(value, (0, 1, 0, 1, 2, 0), last).astype(BF16)
        across = dots(about[0:3], about[3:6])
        value = jnp.concatenate([-about[3:6], -about[0:3], one, none], axis=0)
        last = [*split3(across), pad]
        if fine:
            across_rows[...] = stack(value, (0, 1, 0, 1, 2, 0), last).T.astype(BF16)
            columns = own.T
            for c in range(3):
                target[c] = jnp.broadcast_to(columns[:, c : c + 1], (act, 128))
        else:
            feature[:, act : 2 * act] = stack(value, (0, 1, 0, 1, 2, 0), last).astype(BF16)
        total[...] = jnp.zeros_like(total)

        right[...] = jnp.zeros_like(right)

        @pl.loop(0, half)
        def _(order):
            source = chip_at(order)

            @pl.when(order == 0)
            def _():
                arrival(step, partner, 1, chip).wait_recv()

            @pl.when(order > 0)
            def _():
                arrival(step, 2 * source, 2, source).wait_recv()

            reduce(fine)
            prepare(step, source, centre, fine)
            weigh(step, source, fine)

        reduce(fine)
        plain, scaled = [total[k][0:8] + total[k][8:16] + total[k][16:24] for k in range(2)]
        accel = plain[0:3] - about[0:3] * plain[6:7]
        jerk = (
            plain[3:6]
            - about[3:6] * plain[6:7]
            - 3.0 * (scaled[0:3] - about[0:3] * scaled[6:7])
        )
        return accel, jerk

    pos, vel = own[0:3], own[3:6]
    accel, jerk = field(0, own)
    h = TIME_STEP
    for step in range(STEPS):
        pred_pos = pos + h * vel + h**2 / 2.0 * accel + h**3 / 6.0 * jerk
        pred_vel = vel + h * accel + h**2 / 2.0 * jerk
        accel_new, jerk_new = field(
            step + 1, jnp.concatenate([pred_pos, pred_vel, mass_rows], axis=0)
        )
        vel_new = vel + h / 2.0 * (accel + accel_new) + h**2 / 12.0 * (jerk - jerk_new)
        pos = pos + h / 2.0 * (vel + vel_new) + h**2 / 12.0 * (accel - accel_new)
        vel, accel, jerk = vel_new, accel_new, jerk_new
    out_ref[...] = jnp.concatenate([pos, vel, accel, jerk], axis=0)

    for step in range(STEPS + 1):
        arrival(step, 0, n - 1, 0).wait_send()


def solution(mesh):
    n = mesh.shape["blk"]

    def shards(positions, velocities, masses, active):
        act, stars = active.shape[0], masses.shape[0]
        hbm = pl.BlockSpec(memory_space=pltpu.HBM)
        positions, velocities, masses, active = [
            pltpu.with_memory_space_constraint(value, pltpu.HBM)
            for value in (positions, velocities, masses.reshape(1, -1), active.reshape(1, -1))
        ]
        packed = pl.pallas_call(
            functools.partial(kernel, n),
            out_shape=jax.ShapeDtypeStruct((12, act), F32),
            in_specs=[hbm] * 4,
            out_specs=pl.BlockSpec(memory_space=pltpu.VMEM),
            scratch_shapes=[
                pltpu.VMEM((3, stars), F32),
                pltpu.VMEM((3, stars), F32),
                pltpu.VMEM((1, stars), F32),
                pltpu.VMEM((1, act), jnp.int32),
                pltpu.VMEM((STEPS + 1, n, 8, act), F32),
                pltpu.VMEM((3, act, 128), F32),
                pltpu.VMEM((act, 64), BF16),
                pltpu.VMEM((64, 2 * act), BF16),
                pltpu.VMEM((2, act, 2 * act), F32),
                pltpu.VMEM((4, 2, act, act), BF16),
                pltpu.VMEM((2, 24, act), BF16),
                pltpu.VMEM((2, 24, act), F32),
                pltpu.SemaphoreType.DMA((4,)),
                pltpu.SemaphoreType.DMA((STEPS + 1,)),
                pltpu.SemaphoreType.DMA((STEPS + 1, n // 2)),
            ],
            compiler_params=pltpu.CompilerParams(
                collective_id=0,
                has_side_effects=True,
                vmem_limit_bytes=24 * 1024 * 1024,

            ),
        )(positions, velocities, masses, active)
        return packed[0:3], packed[3:6], packed[6:9], packed[9:12]

    spec = P(None, ("clusters", "blk"))
    flat = P(("clusters", "blk"))
    return jax.shard_map(
        shards,
        mesh=mesh,
        in_specs=(spec, spec, flat, flat),
        out_specs=(spec, spec, spec, spec),
        check_vma=False,
    )
```

```python
import functools

import jax
import jax.numpy as jnp
from jax import lax
from jax.experimental import pallas as pl
from jax.experimental.pallas import tpu as pltpu
from jax.sharding import PartitionSpec as P

STEPS = 2
TIME_STEP = 0.03125
ROWS = 16
SOFT = 0.0025
F32 = jnp.float32
BF16 = jnp.bfloat16


def split3(value):
    high = value.astype(BF16).astype(F32)
    rest = value - high
    middle = rest.astype(BF16).astype(F32)
    return high, middle, rest - middle


def kernel(
    n,
    pos_hbm,
    vel_hbm,
    mass_hbm,
    idx_hbm,
    out_ref,
    pos_ref,
    vel_ref,
    mass_ref,
    idx_ref,
    slots,
    target,
    across_rows,
    feature,
    product,
    weights,
    right,
    total,
    in_sem,
    send_sem,
    recv_sem,
):
    me = lax.axis_index("blk")
    act = idx_ref.shape[1]
    stars = pos_ref.shape[1]

    half = n // 2
    chip = me // 2
    partner = me + 1 - 2 * lax.rem(me, 2)

    barrier = pltpu.get_barrier_semaphore()
    for k in range(1, n):
        pl.semaphore_signal(
            barrier,
            inc=1,
            device_id={"blk": lax.rem(me + k, n)},
            device_id_type=pl.DeviceIdType.MESH,
        )

    loads = [
        pltpu.make_async_copy(source, place, in_sem.at[k])
        for k, (source, place) in enumerate(
            [(idx_hbm, idx_ref), (pos_hbm, pos_ref), (vel_hbm, vel_ref), (mass_hbm, mass_ref)]
        )
    ]
    for load in loads:
        load.start()
    for load in loads:
        load.wait()

    row_id = lax.broadcasted_iota(jnp.int32, (8, act), 0)
    weights[...] = jnp.zeros_like(weights)

    local_idx = idx_ref[...] - me * stars
    table = jnp.concatenate(
        [pos_ref[...], vel_ref[...], mass_ref[...], jnp.zeros((1, stars), F32)], axis=0
    )
    pieces = jnp.concatenate(split3(table), axis=0).astype(BF16)
    picked = (lax.broadcasted_iota(jnp.int32, (stars, act), 0) == local_idx).astype(F32).astype(BF16)
    found = jnp.dot(pieces, picked, preferred_element_type=F32)
    own = found[0:8] + found[8:16] + found[16:24]
    mass_rows = own[6:8]

    def chip_at(order):
        low = jnp.minimum(chip, half - 1 - chip)
        both = chip + ((order + 1) // 2) * (2 * lax.rem(order, 2) - 1)
        side = jnp.where(chip <= half - 1 - chip, order, half - 1 - order)
        return jnp.where(order <= 2 * low, both, side)

    peers = [2 * chip_at(order) for order in range(1, half)]

    def rows_at(step):
        return slice(0, 7 if step == 0 else 6)

    def send(step, peer):
        block = slots.at[step, me, rows_at(step)]
        return pltpu.make_async_remote_copy(
            src_ref=block,
            dst_ref=block,
            send_sem=send_sem.at[step],
            recv_sem=recv_sem.at[step, chip],
            device_id={"blk": peer},
            device_id_type=pl.DeviceIdType.MESH,
        )

    def arrival(step, first, count, source):
        blocks = slots.at[step, pl.ds(first, count), rows_at(step)]
        return pltpu.make_async_remote_copy(
            src_ref=blocks,
            dst_ref=blocks,
            send_sem=send_sem.at[step],
            recv_sem=recv_sem.at[step, source],
            device_id={"blk": partner},
            device_id_type=pl.DeviceIdType.MESH,
        )

    def dots(a, b):
        terms = a * b
        return terms[0:1] + terms[1:2] + terms[2:3]

    def stack(value, order, last):
        parts = split3(value)
        return jnp.concatenate([parts[k] for k in order] + last, axis=0)

    def prepare(step, source, centre, fine):
        for side in range(2):
            about = jnp.where(row_id < 6, slots[step, 2 * source + side] - centre, 0.0)
            factor = jnp.where(row_id == 6, 1.0, about)
            mass = slots[0, 2 * source + side, 6:7]
            right[side] = jnp.concatenate(split3(factor * mass), axis=0).astype(BF16)
            across = dots(about[0:3], about[3:6])
            square = dots(about[0:3], about[0:3])
            about = jnp.where(row_id == 6, across, jnp.where(row_id == 7, square, about))
            near = stack(about, (0, 0, 1, 1, 0, 2), [jnp.ones_like(about), jnp.zeros_like(about)])
            if fine:
                product[side, :, 0:act] = jnp.dot(
                    across_rows[...], near.astype(BF16), preferred_element_type=F32
                )
            else:
                product[side] = jnp.dot(
                    near.astype(BF16).T, feature[...], preferred_element_type=F32
                )

    def weigh(step, source, fine):
        for side in range(2):
            for top in range(0, act, ROWS):
                rows = slice(top, top + ROWS)
                for left in range(0, act, 128):
                    lanes = slice(left, left + 128)
                    if fine:
                        d = [
                            slots[step, 2 * source + side, c : c + 1, lanes] - target[c, rows, :]
                            for c in range(3)
                        ]
                        squared = d[0] * d[0] + d[1] * d[1] + (d[2] * d[2] + SOFT)
                        radial = product[side, rows, lanes]
                    else:
                        squared = product[side, rows, lanes]
                        radial = product[side, rows, act + left : act + left + 128]
                    inverse = lax.rsqrt(squared)
                    inverse2 = inverse * inverse
                    w = inverse2 * inverse
                    z = w * inverse2 * radial
                    for k, value in enumerate([w, z]):
                        high = value.astype(BF16)
                        weights[k, side, rows, lanes] = high
                        if fine:
                            low = (value - high.astype(F32)).astype(BF16)
                            weights[2 + k, side, rows, lanes] = low

    def reduce(fine):
        for side in range(2):
            for k in range(4 if fine else 2):
                total[k % 2] += lax.dot_general(
                    right[side],
                    weights[k, side],
                    (((1,), (1 if fine else 0,)), ((), ())),
                    preferred_element_type=F32,
                )

    def field(step, own):
        fine = step == STEPS
        slots[step, me] = own
        if step == 0:
            pl.semaphore_wait(barrier, n - 1)
        send(step, partner).start()
        for there in peers:
            send(step, there).start()
            send(step, there + 1).start()

        centre = jnp.where(row_id[:, 0:1] < 6, jnp.mean(own, axis=1, keepdims=True), 0.0)
        about = own - centre
        none, one = jnp.zeros((1, act), F32), jnp.ones((1, act), F32)
        pad = jnp.zeros((13, act), F32)
        if not fine:
            square = dots(about[0:3], about[0:3]) + SOFT
            value = jnp.concatenate([-2.0 * about[0:3], none, none, none, none, one], axis=0)
            last = [*split3(square), pad]
            feature[:, 0:act] = stack(value, (0, 1, 0, 1, 2, 0), last).astype(BF16)
        across = dots(about[0:3], about[3:6])
        value = jnp.concatenate([-about[3:6], -about[0:3], one, none], axis=0)
        last = [*split3(across), pad]
        if fine:
            across_rows[...] = stack(value, (0, 1, 0, 1, 2, 0), last).T.astype(BF16)
            columns = own.T
            for c in range(3):
                target[c] = jnp.broadcast_to(columns[:, c : c + 1], (act, 128))
        else:
            feature[:, act : 2 * act] = stack(value, (0, 1, 0, 1, 2, 0), last).astype(BF16)
        total[...] = jnp.zeros_like(total)

        right[...] = jnp.zeros_like(right)

        @pl.loop(0, half)
        def _(order):
            source = chip_at(order)

            @pl.when(order == 0)
            def _():
                arrival(step, partner, 1, chip).wait_recv()

            @pl.when(order > 0)
            def _():
                arrival(step, 2 * source, 2, source).wait_recv()

            reduce(fine)
            prepare(step, source, centre, fine)
            weigh(step, source, fine)

        reduce(fine)
        plain, scaled = [total[k][0:8] + total[k][8:16] + total[k][16:24] for k in range(2)]
        accel = plain[0:3] - about[0:3] * plain[6:7]
        jerk = (
            plain[3:6]
            - about[3:6] * plain[6:7]
            - 3.0 * (scaled[0:3] - about[0:3] * scaled[6:7])
        )
        return accel, jerk

    pos, vel = own[0:3], own[3:6]
    accel, jerk = field(0, own)
    h = TIME_STEP
    for step in range(STEPS):
        pred_pos = pos + h * vel + h**2 / 2.0 * accel + h**3 / 6.0 * jerk
        pred_vel = vel + h * accel + h**2 / 2.0 * jerk
        accel_new, jerk_new = field(
            step + 1, jnp.concatenate([pred_pos, pred_vel, mass_rows], axis=0)
        )
        vel_new = vel + h / 2.0 * (accel + accel_new) + h**2 / 12.0 * (jerk - jerk_new)
        pos = pos + h / 2.0 * (vel + vel_new) + h**2 / 12.0 * (accel - accel_new)
        vel, accel, jerk = vel_new, accel_new, jerk_new
    out_ref[...] = jnp.concatenate([pos, vel, accel, jerk], axis=0)

    for step in range(STEPS + 1):
        arrival(step, 0, n - 1, 0).wait_send()


def solution(mesh):
    n = mesh.shape["blk"]

    def shards(positions, velocities, masses, active):
        act, stars = active.shape[0], masses.shape[0]
        hbm = pl.BlockSpec(memory_space=pltpu.HBM)
        positions, velocities, masses, active = [
            pltpu.with_memory_space_constraint(value, pltpu.HBM)
            for value in (positions, velocities, masses.reshape(1, -1), active.reshape(1, -1))
        ]
        packed = pl.pallas_call(
            functools.partial(kernel, n),
            out_shape=jax.ShapeDtypeStruct((12, act), F32),
            in_specs=[hbm] * 4,
            out_specs=pl.BlockSpec(memory_space=pltpu.VMEM),
            scratch_shapes=[
                pltpu.VMEM((3, stars), F32),
                pltpu.VMEM((3, stars), F32),
                pltpu.VMEM((1, stars), F32),
                pltpu.VMEM((1, act), jnp.int32),
                pltpu.VMEM((STEPS + 1, n, 8, act), F32),
                pltpu.VMEM((3, act, 128), F32),
                pltpu.VMEM((act, 64), BF16),
                pltpu.VMEM((64, 2 * act), BF16),
                pltpu.VMEM((2, act, 2 * act), F32),
                pltpu.VMEM((4, 2, act, act), BF16),
                pltpu.VMEM((2, 24, act), BF16),
                pltpu.VMEM((2, 24, act), F32),
                pltpu.SemaphoreType.DMA((4,)),
                pltpu.SemaphoreType.DMA((STEPS + 1,)),
                pltpu.SemaphoreType.DMA((STEPS + 1, n // 2)),
            ],
            compiler_params=pltpu.CompilerParams(
                collective_id=0,
                has_side_effects=True,
                vmem_limit_bytes=24 * 1024 * 1024,

            ),
        )(positions, velocities, masses, active)
        return packed[0:3], packed[3:6], packed[6:9], packed[9:12]

    spec = P(None, ("clusters", "blk"))
    flat = P(("clusters", "blk"))
    return jax.shard_map(
        shards,
        mesh=mesh,
        in_specs=(spec, spec, flat, flat),
        out_specs=(spec, spec, spec, spec),
        check_vma=False,
    )
```

```python
import functools

import jax
import jax.numpy as jnp
from jax import lax
from jax.experimental import pallas as pl
from jax.experimental.pallas import tpu as pltpu
from jax.sharding import PartitionSpec as P

STEPS = 2
TIME_STEP = 0.03125
ROWS = 16
SOFT = 0.0025
F32 = jnp.float32
BF16 = jnp.bfloat16


def split3(value):
    high = value.astype(BF16).astype(F32)
    rest = value - high
    middle = rest.astype(BF16).astype(F32)
    return high, middle, rest - middle


def kernel(
    n,
    pos_hbm,
    vel_hbm,
    mass_hbm,
    idx_hbm,
    out_ref,
    pos_ref,
    vel_ref,
    mass_ref,
    idx_ref,
    slots,
    target,
    across_rows,
    feature,
    product,
    weights,
    right,
    total,
    in_sem,
    send_sem,
    recv_sem,
):
    me = lax.axis_index("blk")
    act = idx_ref.shape[1]
    stars = pos_ref.shape[1]

    half = n // 2
    chip = me // 2
    partner = me + 1 - 2 * lax.rem(me, 2)

    barrier = pltpu.get_barrier_semaphore()
    for k in range(1, n):
        pl.semaphore_signal(
            barrier,
            inc=1,
            device_id={"blk": lax.rem(me + k, n)},
            device_id_type=pl.DeviceIdType.MESH,
        )

    loads = [
        pltpu.make_async_copy(source, place, in_sem.at[k])
        for k, (source, place) in enumerate(
            [(idx_hbm, idx_ref), (pos_hbm, pos_ref), (vel_hbm, vel_ref), (mass_hbm, mass_ref)]
        )
    ]
    for load in loads:
        load.start()
    for load in loads:
        load.wait()

    row_id = lax.broadcasted_iota(jnp.int32, (8, act), 0)
    weights[...] = jnp.zeros_like(weights)

    local_idx = idx_ref[...] - me * stars
    table = jnp.concatenate(
        [pos_ref[...], vel_ref[...], mass_ref[...], jnp.zeros((1, stars), F32)], axis=0
    )
    pieces = jnp.concatenate(split3(table), axis=0).astype(BF16)
    picked = (lax.broadcasted_iota(jnp.int32, (stars, act), 0) == local_idx).astype(F32).astype(BF16)
    found = jnp.dot(pieces, picked, preferred_element_type=F32)
    own = found[0:8] + found[8:16] + found[16:24]
    mass_rows = own[6:8]

    def chip_at(order):
        low = jnp.minimum(chip, half - 1 - chip)
        both = chip + ((order + 1) // 2) * (2 * lax.rem(order, 2) - 1)
        side = jnp.where(chip <= half - 1 - chip, order, half - 1 - order)
        return jnp.where(order <= 2 * low, both, side)

    peers = [2 * chip_at(order) for order in range(1, half)]

    def rows_at(step):
        return slice(0, 7 if step == 0 else 6)

    def send(step, peer):
        block = slots.at[step, me, rows_at(step)]
        return pltpu.make_async_remote_copy(
            src_ref=block,
            dst_ref=block,
            send_sem=send_sem.at[step],
            recv_sem=recv_sem.at[step, chip],
            device_id={"blk": peer},
            device_id_type=pl.DeviceIdType.MESH,
        )

    def arrival(step, first, count, source):
        blocks = slots.at[step, pl.ds(first, count), rows_at(step)]
        return pltpu.make_async_remote_copy(
            src_ref=blocks,
            dst_ref=blocks,
            send_sem=send_sem.at[step],
            recv_sem=recv_sem.at[step, source],
            device_id={"blk": partner},
            device_id_type=pl.DeviceIdType.MESH,
        )

    def dots(a, b):
        terms = a * b
        return terms[0:1] + terms[1:2] + terms[2:3]

    def stack(value, order, last):
        parts = split3(value)
        return jnp.concatenate([parts[k] for k in order] + last, axis=0)

    def prepare(step, source, centre, fine):
        for side in range(2):
            about = jnp.where(row_id < 6, slots[step, 2 * source + side] - centre, 0.0)
            factor = jnp.where(row_id == 6, 1.0, about)
            mass = slots[0, 2 * source + side, 6:7]
            right[side] = jnp.concatenate(split3(factor * mass), axis=0).astype(BF16)
            across = dots(about[0:3], about[3:6])
            square = dots(about[0:3], about[0:3])
            about = jnp.where(row_id == 6, across, jnp.where(row_id == 7, square, about))
            near = stack(about, (0, 0, 1, 1, 0, 2), [jnp.ones_like(about), jnp.zeros_like(about)])
            if fine:
                product[side, :, 0:act] = jnp.dot(
                    across_rows[...], near.astype(BF16), preferred_element_type=F32
                )
            else:
                product[side] = jnp.dot(
                    near.astype(BF16).T, feature[...], preferred_element_type=F32
                )

    def weigh(step, source, fine, sides=(0, 1)):
        for side in sides:
            for top in range(0, act, ROWS):
                rows = slice(top, top + ROWS)
                for left in range(0, act, 128):
                    lanes = slice(left, left + 128)
                    if fine:
                        d = [
                            slots[step, 2 * source + side, c : c + 1, lanes] - target[c, rows, :]
                            for c in range(3)
                        ]
                        squared = d[0] * d[0] + d[1] * d[1] + (d[2] * d[2] + SOFT)
                        radial = product[side, rows, lanes]
                    else:
                        squared = product[side, rows, lanes]
                        radial = product[side, rows, act + left : act + left + 128]
                    inverse = lax.rsqrt(squared)
                    inverse2 = inverse * inverse
                    w = inverse2 * inverse
                    z = w * inverse2 * radial
                    for k, value in enumerate([w, z]):
                        high = value.astype(BF16)
                        weights[k, side, rows, lanes] = high
                        if fine:
                            low = (value - high.astype(F32)).astype(BF16)
                            weights[2 + k, side, rows, lanes] = low

    def reduce(fine, sides=(0, 1)):
        for side in sides:
            for k in range(4 if fine else 2):
                total[k % 2] += lax.dot_general(
                    right[side],
                    weights[k, side],
                    (((1,), (1 if fine else 0,)), ((), ())),
                    preferred_element_type=F32,
                )

    def field(step, own):
        fine = step == STEPS
        slots[step, me] = own
        if step == 0:
            pl.semaphore_wait(barrier, n - 1)
        send(step, partner).start()
        for there in peers:
            send(step, there).start()
            send(step, there + 1).start()

        centre = jnp.where(row_id[:, 0:1] < 6, jnp.mean(own, axis=1, keepdims=True), 0.0)
        about = own - centre
        none, one = jnp.zeros((1, act), F32), jnp.ones((1, act), F32)
        pad = jnp.zeros((13, act), F32)
        if not fine:
            square = dots(about[0:3], about[0:3]) + SOFT
            value = jnp.concatenate([-2.0 * about[0:3], none, none, none, none, one], axis=0)
            last = [*split3(square), pad]
            feature[:, 0:act] = stack(value, (0, 1, 0, 1, 2, 0), last).astype(BF16)
        across = dots(about[0:3], about[3:6])
        value = jnp.concatenate([-about[3:6], -about[0:3], one, none], axis=0)
        last = [*split3(across), pad]
        if fine:
            across_rows[...] = stack(value, (0, 1, 0, 1, 2, 0), last).T.astype(BF16)
            columns = own.T
            for c in range(3):
                target[c] = jnp.broadcast_to(columns[:, c : c + 1], (act, 128))
        else:
            feature[:, act : 2 * act] = stack(value, (0, 1, 0, 1, 2, 0), last).astype(BF16)
        total[...] = jnp.zeros_like(total)

        right[...] = jnp.zeros_like(right)

        @pl.loop(0, half - 1 if fine else half)
        def _(order):
            source = chip_at(order)

            @pl.when(order == 0)
            def _():
                arrival(step, partner, 1, chip).wait_recv()

            @pl.when(order > 0)
            def _():
                arrival(step, 2 * source, 2, source).wait_recv()

            reduce(fine)
            prepare(step, source, centre, fine)
            weigh(step, source, fine)

        if fine:
            source = peers[-1] // 2
            arrival(step, 2 * source, 2, source).wait_recv()
            reduce(fine)
            prepare(step, source, centre, fine)
            weigh(step, source, fine, (0,))
            reduce(fine, (0,))
            weigh(step, source, fine, (1,))
            reduce(fine, (1,))
        else:
            reduce(fine)
        plain, scaled = [total[k][0:8] + total[k][8:16] + total[k][16:24] for k in range(2)]
        accel = plain[0:3] - about[0:3] * plain[6:7]
        jerk = (
            plain[3:6]
            - about[3:6] * plain[6:7]
            - 3.0 * (scaled[0:3] - about[0:3] * scaled[6:7])
        )
        return accel, jerk

    pos, vel = own[0:3], own[3:6]
    accel, jerk = field(0, own)
    h = TIME_STEP
    for step in range(STEPS):
        pred_pos = pos + h * vel + h**2 / 2.0 * accel + h**3 / 6.0 * jerk
        pred_vel = vel + h * accel + h**2 / 2.0 * jerk
        accel_new, jerk_new = field(
            step + 1, jnp.concatenate([pred_pos, pred_vel, mass_rows], axis=0)
        )
        vel_new = vel + h / 2.0 * (accel + accel_new) + h**2 / 12.0 * (jerk - jerk_new)
        pos = pos + h / 2.0 * (vel + vel_new) + h**2 / 12.0 * (accel - accel_new)
        vel, accel, jerk = vel_new, accel_new, jerk_new
    out_ref[...] = jnp.concatenate([pos, vel, accel, jerk], axis=0)

    for step in range(STEPS + 1):
        arrival(step, 0, n - 1, 0).wait_send()


def solution(mesh):
    n = mesh.shape["blk"]

    def shards(positions, velocities, masses, active):
        act, stars = active.shape[0], masses.shape[0]
        hbm = pl.BlockSpec(memory_space=pltpu.HBM)
        positions, velocities, masses, active = [
            pltpu.with_memory_space_constraint(value, pltpu.HBM)
            for value in (positions, velocities, masses.reshape(1, -1), active.reshape(1, -1))
        ]
        packed = pl.pallas_call(
            functools.partial(kernel, n),
            out_shape=jax.ShapeDtypeStruct((12, act), F32),
            in_specs=[hbm] * 4,
            out_specs=pl.BlockSpec(memory_space=pltpu.VMEM),
            scratch_shapes=[
                pltpu.VMEM((3, stars), F32),
                pltpu.VMEM((3, stars), F32),
                pltpu.VMEM((1, stars), F32),
                pltpu.VMEM((1, act), jnp.int32),
                pltpu.VMEM((STEPS + 1, n, 8, act), F32),
                pltpu.VMEM((3, act, 128), F32),
                pltpu.VMEM((act, 64), BF16),
                pltpu.VMEM((64, 2 * act), BF16),
                pltpu.VMEM((2, act, 2 * act), F32),
                pltpu.VMEM((4, 2, act, act), BF16),
                pltpu.VMEM((2, 24, act), BF16),
                pltpu.VMEM((2, 24, act), F32),
                pltpu.SemaphoreType.DMA((4,)),
                pltpu.SemaphoreType.DMA((STEPS + 1,)),
                pltpu.SemaphoreType.DMA((STEPS + 1, n // 2)),
            ],
            compiler_params=pltpu.CompilerParams(
                collective_id=0,
                has_side_effects=True,
                vmem_limit_bytes=24 * 1024 * 1024,

            ),
        )(positions, velocities, masses, active)
        return packed[0:3], packed[3:6], packed[6:9], packed[9:12]

    spec = P(None, ("clusters", "blk"))
    flat = P(("clusters", "blk"))
    return jax.shard_map(
        shards,
        mesh=mesh,
        in_specs=(spec, spec, flat, flat),
        out_specs=(spec, spec, spec, spec),
        check_vma=False,
    )
```
